32 devices in a mesh: grp: 2 (over x), seq: 16 (over z, y, core).
Axes of the slice: x: 2, y: 2, z: 4, core: 2. Of those that a mesh axis runs over, the one named last changes fastest.
Arguments:
- queries: bfloat16 [512, 4096], P(('grp', 'seq')), parts along dimension 0, may hold values from -36 to 36
- new_keys: bfloat16 [512, 1024], P(('grp', 'seq')), parts along dimension 0, may hold values from -24 to 24
- new_values: bfloat16 [512, 1024], P(('grp', 'seq')), parts along dimension 0, may hold values from -12 to 12
- suffix_keys: bfloat16 [512, 256, 1024], P(('grp', 'seq')), parts along dimension 0, may hold values from -18 to 18
- suffix_values: bfloat16 [512, 256, 1024], P(('grp', 'seq')), parts along dimension 0, may hold values from -12 to 12
- suffix_lens: int32 [512], P(('grp', 'seq')), parts along dimension 0, may hold values from 1 to 256, 32768 in all
- prefix_keys: bfloat16 [2048, 16, 1024], P(('grp', 'seq')), parts along dimension 0, may hold values from -12 to 12
- prefix_values: bfloat16 [2048, 16, 1024], P(('grp', 'seq')), parts along dimension 0, may hold values from -12 to 12
- page_table: int32 [4, 512], P('grp'), parts along dimension 0, may hold values from 0 to 1023, as said below
- prefix_id: int32 [512], P('grp'), parts along dimension 0, may hold values from 0 to 1
Outputs:
- attn_out: bfloat16 [512, 4096], P(('grp', 'seq')), parts along dimension 0
The draws below stay inside these ranges and needn't reach their ends.
There are 2 independent parts, one for each index of `grp`. The reference program is written for one: setup_inputs(seed, part) draws one part's arguments, and reference() takes and returns one part's arrays. A program takes and returns all parts, laid end to end along the dimension named above; each array names one. Nothing has to cross between parts.
Inputs may be any that keep to these rules, and one draw needn't show every extreme that they name: `page_table`: every page id 0 to 1023 stands exactly once in the table. Each run of 64 page ids that starts at a multiple of 64 holds at least one page of every prefix.
All inputs are finite; a program needn't handle non-finite values. No bound on the sum of `suffix_lens` on one device may be relied on, other than what follows from the above.
Results may differ from the reference program's by a relative error of at most 0.005.
Values may be sent and summed in bfloat16 or wider, within the bound.
A program may use at most 192 MiB of HBM per device.

```python
import math
import jax
import jax.numpy as jnp
import numpy as np
from jax import lax

H = 32
KV = 8
HD = 128
NPREF = 2
PAGE = 16
PAGES_DEV = 64
B_DEV = 16
SUF = 256
B = 256
PAGES = 1024
PPP = 512
N_SEQ = 16


def shared_keys(key):
    raw_keys = 4.0 * jax.random.normal(jax.random.fold_in(key, 11), (B, KV * HD), jnp.float32)
    return jnp.clip(raw_keys, -24.0, 24.0)


def draw_new_keys(key, part):
    return shared_keys(key).astype(jnp.bfloat16)


def draw_queries(key, part):
    plain_draw = jnp.clip(jax.random.normal(jax.random.fold_in(key, 12), (B, H * HD), jnp.float32), -6.0, 6.0)
    return plain_draw.astype(jnp.bfloat16)


def draw_page_table(key, part):
    owner_count = PAGES // PAGES_DEV
    spare_slots = PAGES_DEV - NPREF
    leftover = jnp.repeat(jnp.arange(NPREF, dtype=jnp.int32), PPP - owner_count)
    leftover = jax.random.permutation(jax.random.fold_in(key, 3), leftover).reshape(owner_count, spare_slots)
    base_rows = jnp.tile(jnp.arange(NPREF, dtype=jnp.int32)[None, :], (owner_count, 1))
    labels = jnp.concatenate([base_rows, leftover], axis=1)
    labels = jax.random.permutation(jax.random.fold_in(key, 4), labels, axis=1, independent=True)
    order_list = jnp.argsort(labels.reshape(-1), stable=True)
    return order_list.reshape(NPREF, PPP).astype(jnp.int32)


def set_ends(drawn, stream_key, smallest, high):
    dims = drawn.shape
    spot = [jax.random.randint(jax.random.fold_in(stream_key, axis), (), 0, dims[axis]) for axis in range(len(dims))]
    drawn = drawn.at[tuple(spot)].set(smallest)
    longest = dims.index(max(dims))
    spot[longest] = (spot[longest] + 1) % dims[longest]
    return drawn.at[tuple(spot)].set(high)


def block_levels(key, dims, cuts, least, high):
    loudness, own = 1.0, jax.random.fold_in(key, 6)
    for dim, parts in cuts:
        draws = jnp.exp(jax.random.uniform(jax.random.fold_in(own, dim), (parts,), jnp.float32, least / len(cuts), high / len(cuts)))
        loudness = loudness * jnp.repeat(draws, dims[dim] // parts).reshape([-1 if axis == dim else 1 for axis in range(len(dims))])
    return loudness


def rank_bounds(number_of, skew):
    loads = [(1 << 20) // math.isqrt(standing ** skew) + 1 for standing in range(1, number_of + 1)]
    deviation = 1 + sum(loads) // (1 << 30)
    return np.cumsum(np.array([max(1, weight // deviation) for weight in loads]))


def ranked_ids(rng, extent, count, skew):
    table = rank_bounds(count, skew)
    lot = jax.random.randint(jax.random.fold_in(rng, 1), extent, 0, int(table[count - 1]))
    rank = jnp.searchsorted(jnp.asarray(table, jnp.int32), lot, side="right")
    return jax.random.permutation(jax.random.fold_in(rng, 2), count)[rank].astype(jnp.int32)


def split_up(count, total, most, skew):
    loads = [(1 << 20) // math.isqrt(standing ** skew) + 1 for standing in range(2, count + 1)]
    spare, counts = total - most - (count - 1), [1] * (count - 1)
    while spare > 0:
        free = [i for i in range(count - 1) if counts[i] < most]
        whole, remaining = sum([loads[i] for i in free]), spare
        for i in free:
            extra = min(most - counts[i], max(1, remaining * loads[i] // whole), spare)
            counts[i] = counts[i] + extra
            spare = spare - extra
    return np.array([most] + counts)


def ragged_sizes(key, count, total, reach, lean):
    if count == 2:
        one = jax.random.randint(key, (), max(1, total - reach), min(reach, total - 1) + 1)
        return jnp.stack([one, total - one])
    tallies = jnp.asarray(split_up(count, total, reach, lean), jnp.int32)
    couples = (count - 1) // 2
    source_of, taker = tallies[1:1 + 2 * couples:2], tallies[2:2 + 2 * couples:2]
    room = jnp.minimum(source_of - 1, reach - taker)
    shifted = jax.random.randint(jax.random.fold_in(key, 1), (couples,), 0, 1 << 20) % (room + 1)
    tallies = tallies.at[1:1 + 2 * couples:2].set(source_of - shifted).at[2:2 + 2 * couples:2].set(taker + shifted)
    return tallies[jax.random.permutation(jax.random.fold_in(key, 2), count)]


def gaussian(rng, dims, width, limit, pieces=(), kind=jnp.bfloat16):
    array = jax.random.normal(rng, dims, jnp.float32) * width
    if len(pieces) > 0:
        array = block_levels(rng, dims, pieces, -0.22, 0.18) * array
    return jnp.clip(array, min=-limit, max=limit).astype(kind)


def setup_inputs(seed: int = 0, part: int = 0) -> dict:
    key_list = jax.random.split(jax.random.key(seed), 11)
    part_splits = jax.random.split(jax.random.fold_in(key_list[10], part), 11)
    return {
        "queries": draw_queries(jax.random.fold_in(jax.random.fold_in(key_list[10], part), 71), part),
        "new_keys": draw_new_keys(jax.random.fold_in(jax.random.fold_in(key_list[10], part), 71), part),
        "new_values": gaussian(part_splits[2], (B, KV * HD), 2.0, 12.0, ((0, 16),)),
        "suffix_keys": gaussian(part_splits[3], (B, SUF, KV * HD), 3.0, 18.0, ((0, 16),)),
        "suffix_values": gaussian(part_splits[4], (B, SUF, KV * HD), 2.0, 12.0, ((0, 16),)),
        "suffix_lens": ragged_sizes(part_splits[5], B, B * SUF // 2, SUF, 2).astype(jnp.int32),
        "prefix_keys": gaussian(part_splits[6], (PAGES, PAGE, KV * HD), 2.0, 12.0, ((0, 16),)),
        "prefix_values": gaussian(part_splits[7], (PAGES, PAGE, KV * HD), 2.0, 12.0, ((0, 16),)),
        "page_table": draw_page_table(jax.random.fold_in(jax.random.fold_in(key_list[10], part), 71), part),
        "prefix_id": set_ends(ranked_ids(part_splits[9], (B,), NPREF, 2), jax.random.fold_in(part_splits[9], 3), 0, NPREF - 1).astype(jnp.int32),
    }


def reference(queries, new_keys, new_values, suffix_keys, suffix_values, suffix_lens, prefix_keys, prefix_values, page_table, prefix_id):
    group_size = H // KV
    softmax_scale = 1.0 / math.sqrt(HD)
    block_tokens = PAGES_DEV * PAGE
    page_ids = jnp.arange(PAGES, dtype=jnp.int32)
    page_hits = jnp.any(page_table[:, :, None] == page_ids[None, None, :], axis=1)
    prefix_of_page = lax.optimization_barrier(jnp.sum(page_hits.astype(jnp.int32) * jnp.arange(NPREF, dtype=jnp.int32)[:, None], axis=0))
    token_label = jnp.repeat(prefix_of_page, PAGE)
    pool_keys = prefix_keys.reshape(PAGES * PAGE, KV, HD).astype(jnp.float32)
    pool_values = prefix_values.reshape(N_SEQ, block_tokens, KV, HD).astype(jnp.float32)
    block_count = B // B_DEV
    slot_index = jnp.arange(SUF, dtype=jnp.int32)

    def one_block(inputs):
        block_queries, block_new_keys, block_new_values, block_suffix_keys, block_suffix_values, block_lens, block_ids = inputs
        query_head_count = block_queries.reshape(B_DEV, KV, group_size, HD).astype(jnp.float32)
        prefix_scores = jnp.einsum('bkgd,tkd->bkgt', query_head_count, pool_keys) * softmax_scale
        prefix_live = (block_ids[:, None] == token_label[None, :])[:, None, None, :]
        prefix_scores = jnp.where(prefix_live, prefix_scores, -1e+30)
        prefix_scores = prefix_scores.reshape(B_DEV, KV, group_size, N_SEQ, block_tokens)
        prefix_live = prefix_live.reshape(B_DEV, 1, 1, N_SEQ, block_tokens)
        block_peak = lax.optimization_barrier(jnp.max(prefix_scores, axis=4))
        block_weights = jnp.where(prefix_live, jnp.exp(prefix_scores - block_peak[..., None]), 0.0)
        block_mass = lax.optimization_barrier(jnp.sum(block_weights, axis=4))
        block_round = lax.optimization_barrier(block_weights.astype(jnp.bfloat16)).astype(jnp.float32)
        block_numer = jnp.einsum('bkgot,otkd->bkgod', block_round, pool_values)
        block_out = block_numer / block_mass[..., None]
        block_out = lax.optimization_barrier(block_out.astype(jnp.bfloat16)).astype(jnp.float32)
        block_lse = block_peak + jnp.log(block_mass)
        own_keys = block_suffix_keys.reshape(B_DEV, SUF, KV, HD).astype(jnp.float32)
        own_values = block_suffix_values.reshape(B_DEV, SUF, KV, HD).astype(jnp.float32)
        suffix_scores = jnp.einsum('bkgd,btkd->bkgt', query_head_count, own_keys) * softmax_scale
        suffix_live = (slot_index[None, :] < block_lens[:, None])[:, None, None, :]
        suffix_scores = jnp.where(suffix_live, suffix_scores, -1e+30)
        incoming_keys = block_new_keys.reshape(B_DEV, KV, HD).astype(jnp.float32)
        incoming_values = block_new_values.reshape(B_DEV, KV, HD).astype(jnp.float32)
        incoming_scores = jnp.einsum('iqnc,iqc->iqn', query_head_count, incoming_keys) * softmax_scale
        home_peak = jnp.maximum(lax.optimization_barrier(jnp.max(suffix_scores, axis=3)), incoming_scores)
        suffix_weights = jnp.where(suffix_live, jnp.exp(suffix_scores - home_peak[..., None]), 0.0)
        fresh_weights = jnp.exp(incoming_scores - home_peak)
        home_mass = lax.optimization_barrier(jnp.sum(suffix_weights, axis=3)) + fresh_weights
        suffix_round = lax.optimization_barrier(suffix_weights.astype(jnp.bfloat16)).astype(jnp.float32)
        incoming_rounded = lax.optimization_barrier(fresh_weights.astype(jnp.bfloat16)).astype(jnp.float32)
        resident_numerator = jnp.einsum('bkgt,btkd->bkgd', suffix_round, own_values)
        resident_numerator = resident_numerator + jnp.einsum('cqx,cqh->cqxh', incoming_rounded, incoming_values)
        home_out = resident_numerator / home_mass[..., None]
        home_lse = home_peak + jnp.log(home_mass)
        overall = jnp.maximum(lax.optimization_barrier(jnp.max(block_lse, axis=3)), home_lse)
        factor = jnp.exp(block_lse - overall[..., None])
        home_factor = jnp.exp(home_lse - overall)
        merged = lax.optimization_barrier(jnp.sum(factor[..., None] * block_out, axis=3)) + home_factor[..., None] * home_out
        divisor = lax.optimization_barrier(jnp.sum(factor, axis=3)) + home_factor
        result = merged / divisor[..., None]
        return result.reshape(B_DEV, H * HD).astype(jnp.bfloat16)
    stacked = (queries.reshape(block_count, B_DEV, H * HD), new_keys.reshape(block_count, B_DEV, KV * HD), new_values.reshape(block_count, B_DEV, KV * HD), suffix_keys.reshape(block_count, B_DEV, SUF, KV * HD), suffix_values.reshape(block_count, B_DEV, SUF, KV * HD), suffix_lens.reshape(block_count, B_DEV), prefix_id.reshape(block_count, B_DEV))
    outputs = lax.map(one_block, stacked)
    return outputs.reshape(B, H * HD)
```

```python
import functools
import math

import jax
import jax.numpy as jnp
from jax import lax
from jax.experimental import pallas as pl
from jax.experimental.pallas import tpu as pltpu
from jax.sharding import PartitionSpec as P

H = 32
KV = 8
HD = 128
NPREF = 2
G = H // KV
MASKED = -1e30
SCALE2 = math.log2(math.e) / math.sqrt(HD)
NT = (((1,), (1,)), ((), ()))


def low_bit(m):
    return m & (-m)


def kernel(
    n,
    q_hbm, nk_ref, nv_ref, sk_hbm, sv_hbm, lens_ref, pk_hbm, pv_hbm, label_ref, onehot_ref,
    out_ref,
    qs, sk, sv, pk, pv, part, lse, recv_o, recv_l, eg, q_rows, home_o, home_l,
    in_sem, suf_sem, ag_send, ag_recv, o_send, o_recv, l_send, l_recv,
):
    rows = q_hbm.shape[0]
    slots = sk.shape[1]
    me = lax.axis_index("seq")

    def flip(bit):
        return me + bit * (1 - 2 * ((me // bit) % 2))

    def xor(m):
        index = me
        bit = 1
        while bit < n:
            if m & bit:
                index = index + bit * (1 - 2 * ((me // bit) % 2))
            bit *= 2
        return index

    bits = [1 << i for i in range(n.bit_length() - 1)]

    q_copy = pltpu.make_async_copy(q_hbm, qs.at[0], in_sem.at[0])
    q_copy.start()
    for b in range(rows):
        pltpu.make_async_copy(sk_hbm.at[b], sk.at[b], suf_sem.at[0, b]).start()
        pltpu.make_async_copy(sv_hbm.at[b], sv.at[b], suf_sem.at[1, b]).start()
    k_copy = pltpu.make_async_copy(pk_hbm, pk, in_sem.at[1])
    v_copy = pltpu.make_async_copy(pv_hbm, pv, in_sem.at[2])
    k_copy.start()
    v_copy.start()

    barrier = pltpu.get_barrier_semaphore()
    for bit in bits:
        pl.semaphore_signal(
            barrier, inc=1, device_id={"seq": flip(bit)},
            device_id_type=pl.DeviceIdType.MESH,
        )
    pl.semaphore_wait(barrier, len(bits))
    q_copy.wait()

    def gather_copy(m):
        bit = low_bit(m)
        return pltpu.make_async_remote_copy(
            src_ref=qs.at[m ^ bit], dst_ref=qs.at[m],
            send_sem=ag_send.at[m], recv_sem=ag_recv.at[m],
            device_id={"seq": flip(bit)}, device_id_type=pl.DeviceIdType.MESH,
        )

    def forward(m):
        limit = n if m == 0 else low_bit(m)
        for bit in reversed(bits):
            if bit < limit:
                gather_copy(m + bit).start()

    arrived = set([0])

    def arrive(m):
        if m not in arrived:
            arrived.add(m)
            arrive(m ^ low_bit(m))
            gather_copy(m).wait_recv()
            forward(m)

    forward(0)

    for h in range(H):
        q_rows[pl.ds(h, rows, stride=H), :] = qs[0, :, h * HD:(h + 1) * HD].astype(jnp.float32)

    row_head = lax.broadcasted_iota(jnp.int32, (H, HD), 0) // G
    slot_iota = lax.broadcasted_iota(jnp.int32, (H, slots), 1)
    new_iota = lax.broadcasted_iota(jnp.int32, (H, rows), 1)

    def suffix(b, carry):
        pltpu.make_async_copy(sk_hbm.at[b], sk.at[b], suf_sem.at[0, b]).wait()
        pltpu.make_async_copy(sv_hbm.at[b], sv.at[b], suf_sem.at[1, b]).wait()
        q = q_rows[pl.ds(b * H, H), :]
        wide = jnp.concatenate(
            [jnp.where(row_head == k, q, 0.0) for k in range(KV)], axis=1
        ).astype(jnp.bfloat16)
        s = lax.dot_general(wide, sk[b], NT, preferred_element_type=jnp.float32)
        s = jnp.where(slot_iota < lens_ref[b], s, MASKED)
        sn = lax.dot_general(wide, nk_ref[...], NT, preferred_element_type=jnp.float32)
        sn = jnp.where(new_iota == b, sn, MASKED)
        peak = jnp.maximum(
            jnp.max(s, axis=1, keepdims=True), jnp.max(sn, axis=1, keepdims=True)
        )
        p = jnp.exp2((s - peak) * SCALE2)
        pn = jnp.exp2((sn - peak) * SCALE2)
        mass = jnp.sum(p, axis=1, keepdims=True) + jnp.sum(pn, axis=1, keepdims=True)
        o = jnp.dot(p.astype(jnp.bfloat16), sv[b], preferred_element_type=jnp.float32)
        o = o + jnp.dot(pn.astype(jnp.bfloat16), nv_ref[...], preferred_element_type=jnp.float32)
        own = jnp.zeros((H, HD), jnp.float32)
        for k in range(KV):
            own = own + jnp.where(row_head == k, o[:, k * HD:(k + 1) * HD], 0.0)
        home_o[pl.ds(b * H, H), :] = own / mass
        home_l[pl.ds(b * H, H), :] = jnp.broadcast_to(
            peak * SCALE2 + jnp.log2(mass), (H, HD)
        )
        return carry

    arrival = sorted(range(1, n), key=lambda m: (bin(m).count("1"), m % 2, m))
    even = [m for m in arrival if m % 2 == 0]
    segments = 4
    cut = [rows * i // segments for i in range(segments + 1)]
    share = [len(even) * i // segments for i in range(segments + 1)]
    for i in range(segments):
        lax.fori_loop(cut[i], cut[i + 1], suffix, 0)
        for m in even[share[i]:share[i + 1]]:
            arrive(m)

    k_copy.wait()
    v_copy.wait()
    lane = lax.broadcasted_iota(jnp.int32, (rows, HD), 1)
    tokens = pk.shape[0]

    def compute(blocks, first, last):
        def head(k, carry):
            base = pl.multiple_of(k * (G * HD), G * HD)
            cols = pl.ds(pl.multiple_of(k * HD, HD), HD)
            q = jnp.concatenate(
                [qs[m, :, pl.ds(base + g * HD, HD)] for m in blocks for g in range(G)], axis=0
            )
            qx = jnp.concatenate([q, eg[...]], axis=1)
            kx = jnp.concatenate([pk[:, cols], label_ref[...]], axis=1)
            s = lax.dot_general(qx, kx, NT, preferred_element_type=jnp.float32)
            peak = jnp.max(s, axis=1, keepdims=True)
            p = jnp.exp2((s - peak) * SCALE2).astype(jnp.bfloat16)
            vx = jnp.concatenate(
                [pv[:, cols], jnp.ones((tokens, HD), jnp.bfloat16)], axis=1
            )
            o = jnp.dot(p, vx, preferred_element_type=jnp.float32)
            mass = o[:, HD:]
            res = (o[:, :HD] / mass).astype(jnp.bfloat16)
            level = peak * SCALE2 + jnp.log2(mass)
            for i, m in enumerate(blocks):
                total = lse[m]
                for g in range(G):
                    at = (i * G + g) * rows
                    part[m, :, pl.ds(base + g * HD, HD)] = res[at:at + rows]
                    total = jnp.where(lane == k * G + g, level[at:at + rows], total)
                lse[m] = total
            return carry

        lax.fori_loop(first, last, head, 0)

    def partner_copies(m):
        where = {"seq": flip(low_bit(m))}
        return [
            pltpu.make_async_remote_copy(
                src_ref=src.at[m], dst_ref=dst.at[m], send_sem=s.at[m], recv_sem=r.at[m],
                device_id=where, device_id_type=pl.DeviceIdType.MESH,
            )
            for src, dst, s, r in ((part, recv_o, o_send, o_recv), (lse, recv_l, l_send, l_recv))
        ]

    def send(m):
        for copy in partner_copies(m):
            copy.start()

    def pick(w, h):
        return jnp.sum(jnp.where(lane == h, w, 0.0), axis=1, keepdims=True)

    def blend(a, b):
        top = jnp.maximum(a, b)
        return 1.0 / (1.0 + jnp.exp2(b - a)), top + jnp.log2(1.0 + jnp.exp2(-jnp.abs(a - b)))

    def merge(m, child):
        for copy in partner_copies(child):
            copy.wait_recv()
        w, level = blend(recv_l[child], lse[m])
        lse[m] = level

        def step(k, carry):
            base = pl.multiple_of(k * (G * HD), G * HD)
            for g in range(G):
                at = pl.ds(base + g * HD, HD)
                a = recv_o[child, :, at].astype(jnp.float32)
                b = part[m, :, at].astype(jnp.float32)
                part[m, :, at] = (b + (a - b) * pick(w, k * G + g)).astype(jnp.bfloat16)
            return carry

        lax.fori_loop(0, KV, step, 0)

    pairs = [m for m in range(0, n, 2)]
    pairs.sort(key=lambda m: (low_bit(m) if m else n, m))
    groups = [pairs[i:i + 2] for i in range(0, len(pairs), 2)]

    def settle(group):
        for m in group:
            if m == 0:
                continue
            bit = 1
            while bit < low_bit(m):
                merge(m, m + bit)
                bit *= 2
            send(m)

    waiting = []
    for group in groups:
        blocks = [m + odd for m in group for odd in (1, 0)]
        for m in blocks:
            arrive(m)
            lse[m] = jnp.zeros((rows, HD), jnp.float32)
        for i, m in enumerate(blocks):
            code = onehot_ref[xor(m)]
            for g in range(G):
                at = (i * G + g) * rows
                eg[at:at + rows] = code
        half = KV // 2
        compute(blocks, 0, half)
        settle(waiting)
        compute(blocks, half, KV)
        for m in blocks:
            if m % 2:
                send(m)
        waiting = group
    settle(waiting)

    for bit in bits[:-1]:
        merge(0, bit)
    last = bits[-1]
    for copy in partner_copies(last):
        copy.wait_recv()
    w, level = blend(recv_l[last], lse[0])

    def finish(k, carry):
        base = pl.multiple_of(k * (G * HD), G * HD)
        for g in range(G):
            h = k * G + g
            at = pl.ds(base + g * HD, HD)
            a = recv_o[last, :, at].astype(jnp.float32)
            b = part[0, :, at].astype(jnp.float32)
            x = b + (a - b) * pick(w, h)
            mine = pl.ds(h, rows, stride=H)
            home = home_o[mine, :]
            w_home = 1.0 / (1.0 + jnp.exp2(pick(level, h) - home_l[mine, :]))
            out_ref[:, at] = (x + (home - x) * w_home).astype(jnp.bfloat16)
        return carry

    lax.fori_loop(0, KV, finish, 0)
    for m in range(1, n):
        gather_copy(m).wait_send()
        for copy in partner_copies(m):
            copy.wait_send()


def local(
    queries, new_keys, new_values, suffix_keys, suffix_values, suffix_lens,
    prefix_keys, prefix_values, page_table, prefix_id,
):
    n = lax.axis_size("seq")
    rows = queries.shape[0]
    slots = suffix_keys.shape[1]
    pages, page, width = prefix_keys.shape
    tokens = pages * page
    ids = lax.axis_index("seq") * pages + jnp.arange(pages, dtype=jnp.int32)
    hits = jnp.any(page_table[:, :, None] == ids[None, None, :], axis=1)
    prefixes = jnp.arange(NPREF, dtype=jnp.int32)
    label = jnp.sum(hits.astype(jnp.int32) * prefixes[:, None], axis=0)
    lanes = jnp.arange(HD, dtype=jnp.int32)
    barred = (lanes[None, :] < NPREF) & (lanes[None, :] != label[:, None])
    label_cols = jnp.where(barred, MASKED, 0.0).astype(jnp.bfloat16)
    label_cols = jnp.broadcast_to(label_cols[:, None, :], (pages, page, HD)).reshape(tokens, HD)
    onehot = (prefix_id.reshape(n, rows, 1) == lanes).astype(jnp.bfloat16)
    vmem = pl.BlockSpec(memory_space=pltpu.VMEM)
    hbm = pl.BlockSpec(memory_space=pl.ANY)
    smem = pl.BlockSpec(memory_space=pltpu.SMEM)
    bf16, f32 = jnp.bfloat16, jnp.float32
    dma = pltpu.SemaphoreType.DMA
    return pl.pallas_call(
        functools.partial(kernel, n),
        out_shape=jax.ShapeDtypeStruct((rows, H * HD), bf16),
        in_specs=[hbm, vmem, vmem, hbm, hbm, smem, hbm, hbm, vmem, vmem],
        out_specs=vmem,
        scratch_shapes=[
            pltpu.VMEM((n, rows, H * HD), bf16),
            pltpu.VMEM((rows, slots, width), bf16),
            pltpu.VMEM((rows, slots, width), bf16),
            pltpu.VMEM((tokens, width), bf16),
            pltpu.VMEM((tokens, width), bf16),
            pltpu.VMEM((n, rows, H * HD), bf16),
            pltpu.VMEM((n, rows, HD), f32),
            pltpu.VMEM((n, rows, H * HD), bf16),
            pltpu.VMEM((n, rows, HD), f32),
            pltpu.VMEM((4 * G * rows, HD), bf16),
            pltpu.VMEM((rows * H, HD), f32),
            pltpu.VMEM((rows * H, HD), f32),
            pltpu.VMEM((rows * H, HD), f32),
            dma((3,)),
            dma((2, rows)),
            dma((n,)), dma((n,)), dma((n,)), dma((n,)), dma((n,)), dma((n,)),
        ],
        compiler_params=pltpu.CompilerParams(
            collective_id=0, has_side_effects=True, vmem_limit_bytes=64 * 1024 * 1024 - 65536,
        ),
        name="step",
    )(
        queries, new_keys, new_values, suffix_keys, suffix_values, suffix_lens,
        prefix_keys.reshape(tokens, width), prefix_values.reshape(tokens, width),
        label_cols, onehot,
    )


def solution(mesh):
    return jax.shard_map(
        local,
        mesh=mesh,
        in_specs=(
            P(("grp", "seq"), None),
            P(("grp", "seq"), None),
            P(("grp", "seq"), None),
            P(("grp", "seq"), None, None),
            P(("grp", "seq"), None, None),
            P(("grp", "seq")),
            P(("grp", "seq"), None, None),
            P(("grp", "seq"), None, None),
            P("grp", None),
            P("grp"),
        ),
        out_specs=P(("grp", "seq"), None),
        check_vma=False,
    )
```

```python
import functools
import math

import jax
import jax.numpy as jnp
from jax import lax
from jax.experimental import pallas as pl
from jax.experimental.pallas import tpu as pltpu
from jax.sharding import PartitionSpec as P

H = 32
KV = 8
HD = 128
NPREF = 2
G = H // KV
MASKED = -1e30
SCALE2 = math.log2(math.e) / math.sqrt(HD)
NT = (((1,), (1,)), ((), ()))


def low_bit(m):
    return m & (-m)


def kernel(
    n,
    q_hbm, nk_ref, nv_ref, sk_hbm, sv_hbm, lens_ref, pk_hbm, pv_hbm, label_ref, onehot_ref,
    out_ref,
    qs, sk, sv, pk, pv, part, lse, recv_o, recv_l, eg, q_rows, home_o, home_l,
    in_sem, suf_sem, ag_send, ag_recv, o_send, o_recv, l_send, l_recv,
):
    rows = q_hbm.shape[0]
    slots = sk.shape[1]
    me = lax.axis_index("seq")

    def flip(bit):
        return me + bit * (1 - 2 * ((me // bit) % 2))

    def xor(m):
        index = me
        bit = 1
        while bit < n:
            if m & bit:
                index = index + bit * (1 - 2 * ((me // bit) % 2))
            bit *= 2
        return index

    bits = [1 << i for i in range(n.bit_length() - 1)]

    q_copy = pltpu.make_async_copy(q_hbm, qs.at[0], in_sem.at[0])
    q_copy.start()
    for b in range(rows):
        pltpu.make_async_copy(sk_hbm.at[b], sk.at[b], suf_sem.at[0, b]).start()
        pltpu.make_async_copy(sv_hbm.at[b], sv.at[b], suf_sem.at[1, b]).start()
    k_copy = pltpu.make_async_copy(pk_hbm, pk, in_sem.at[1])
    v_copy = pltpu.make_async_copy(pv_hbm, pv, in_sem.at[2])
    k_copy.start()
    v_copy.start()

    barrier = pltpu.get_barrier_semaphore()
    for bit in bits:
        pl.semaphore_signal(
            barrier, inc=1, device_id={"seq": flip(bit)},
            device_id_type=pl.DeviceIdType.MESH,
        )
    pl.semaphore_wait(barrier, len(bits))
    q_copy.wait()

    def gather_copy(m):
        bit = low_bit(m)
        return pltpu.make_async_remote_copy(
            src_ref=qs.at[m ^ bit], dst_ref=qs.at[m],
            send_sem=ag_send.at[m], recv_sem=ag_recv.at[m],
            device_id={"seq": flip(bit)}, device_id_type=pl.DeviceIdType.MESH,
        )

    def forward(m):
        limit = n if m == 0 else low_bit(m)
        for bit in reversed(bits):
            if bit < limit:
                gather_copy(m + bit).start()

    arrived = set([0])

    def arrive(m):
        if m not in arrived:
            arrived.add(m)
            arrive(m ^ low_bit(m))
            gather_copy(m).wait_recv()
            forward(m)

    forward(0)

    for h in range(H):
        q_rows[pl.ds(h, rows, stride=H), :] = qs[0, :, h * HD:(h + 1) * HD].astype(jnp.float32)

    row_head = lax.broadcasted_iota(jnp.int32, (H, HD), 0) // G
    slot_iota = lax.broadcasted_iota(jnp.int32, (H, slots), 1)
    new_iota = lax.broadcasted_iota(jnp.int32, (H, rows), 1)

    def suffix(b, carry):
        pltpu.make_async_copy(sk_hbm.at[b], sk.at[b], suf_sem.at[0, b]).wait()
        pltpu.make_async_copy(sv_hbm.at[b], sv.at[b], suf_sem.at[1, b]).wait()
        q = q_rows[pl.ds(b * H, H), :]
        wide = jnp.concatenate(
            [jnp.where(row_head == k, q, 0.0) for k in range(KV)], axis=1
        ).astype(jnp.bfloat16)
        s = lax.dot_general(wide, sk[b], NT, preferred_element_type=jnp.float32)
        s = jnp.where(slot_iota < lens_ref[b], s, MASKED)
        sn = lax.dot_general(wide, nk_ref[...], NT, preferred_element_type=jnp.float32)
        sn = jnp.where(new_iota == b, sn, MASKED)
        peak = jnp.maximum(
            jnp.max(s, axis=1, keepdims=True), jnp.max(sn, axis=1, keepdims=True)
        )
        p = jnp.exp2((s - peak) * SCALE2)
        pn = jnp.exp2((sn - peak) * SCALE2)
        mass = jnp.sum(p, axis=1, keepdims=True) + jnp.sum(pn, axis=1, keepdims=True)
        o = jnp.dot(p.astype(jnp.bfloat16), sv[b], preferred_element_type=jnp.float32)
        o = o + jnp.dot(pn.astype(jnp.bfloat16), nv_ref[...], preferred_element_type=jnp.float32)
        own = jnp.zeros((H, HD), jnp.float32)
        for k in range(KV):
            own = own + jnp.where(row_head == k, o[:, k * HD:(k + 1) * HD], 0.0)
        home_o[pl.ds(b * H, H), :] = own / mass
        home_l[pl.ds(b * H, H), :] = jnp.broadcast_to(
            peak * SCALE2 + jnp.log2(mass), (H, HD)
        )
        return carry

    arrival = sorted(range(1, n), key=lambda m: (bin(m).count("1"), -m if m & (m - 1) else m))
    even = [m for m in arrival if m % 2 == 0]
    segments = 8
    cut = [rows * i // segments for i in range(segments + 1)]
    share = [len(even) * i // segments for i in range(segments + 1)]
    for i in range(segments):
        lax.fori_loop(cut[i], cut[i + 1], suffix, 0)
        for m in even[share[i]:share[i + 1]]:
            arrive(m)

    k_copy.wait()
    v_copy.wait()
    lane = lax.broadcasted_iota(jnp.int32, (rows, HD), 1)
    tokens = pk.shape[0]

    def compute(blocks, first, last):
        def head(k, carry):
            base = pl.multiple_of(k * (G * HD), G * HD)
            cols = pl.ds(pl.multiple_of(k * HD, HD), HD)
            q = jnp.concatenate(
                [qs[m, :, pl.ds(base + g * HD, HD)] for m in blocks for g in range(G)], axis=0
            )
            qx = jnp.concatenate([q, eg[...]], axis=1)
            kx = jnp.concatenate([pk[:, cols], label_ref[...]], axis=1)
            s = lax.dot_general(qx, kx, NT, preferred_element_type=jnp.float32)
            peak = jnp.max(s, axis=1, keepdims=True)
            p = jnp.exp2((s - peak) * SCALE2).astype(jnp.bfloat16)
            vx = jnp.concatenate(
                [pv[:, cols], jnp.ones((tokens, HD), jnp.bfloat16)], axis=1
            )
            o = jnp.dot(p, vx, preferred_element_type=jnp.float32)
            mass = o[:, HD:]
            res = (o[:, :HD] / mass).astype(jnp.bfloat16)
            level = peak * SCALE2 + jnp.log2(mass)
            for i, m in enumerate(blocks):
                total = lse[m]
                for g in range(G):
                    at = (i * G + g) * rows
                    part[m, :, pl.ds(base + g * HD, HD)] = res[at:at + rows]
                    total = jnp.where(lane == k * G + g, level[at:at + rows], total)
                lse[m] = total
            return carry

        lax.fori_loop(first, last, head, 0, unroll=4)

    def partner_copies(m):
        where = {"seq": flip(low_bit(m))}
        return [
            pltpu.make_async_remote_copy(
                src_ref=src.at[m], dst_ref=dst.at[m], send_sem=s.at[m], recv_sem=r.at[m],
                device_id=where, device_id_type=pl.DeviceIdType.MESH,
            )
            for src, dst, s, r in ((part, recv_o, o_send, o_recv), (lse, recv_l, l_send, l_recv))
        ]

    def send(m):
        for copy in partner_copies(m):
            copy.start()

    def pick(w, h):
        return jnp.sum(jnp.where(lane == h, w, 0.0), axis=1, keepdims=True)

    def blend(a, b):
        top = jnp.maximum(a, b)
        return 1.0 / (1.0 + jnp.exp2(b - a)), top + jnp.log2(1.0 + jnp.exp2(-jnp.abs(a - b)))

    def merge(m, child):
        for copy in partner_copies(child):
            copy.wait_recv()
        w, level = blend(recv_l[child], lse[m])
        lse[m] = level

        def step(k, carry):
            base = pl.multiple_of(k * (G * HD), G * HD)
            for g in range(G):
                at = pl.ds(base + g * HD, HD)
                a = recv_o[child, :, at].astype(jnp.float32)
                b = part[m, :, at].astype(jnp.float32)
                part[m, :, at] = (b + (a - b) * pick(w, k * G + g)).astype(jnp.bfloat16)
            return carry

        lax.fori_loop(0, KV, step, 0, unroll=4)

    pairs = [m for m in range(0, n, 2)]
    pairs.sort(key=lambda m: (low_bit(m) != 2, -m))
    groups = [pairs[i:i + 2] for i in range(0, len(pairs), 2)]

    def settle(group):
        for m in group:
            if m == 0:
                continue
            bit = 1
            while bit < low_bit(m):
                merge(m, m + bit)
                bit *= 2
            send(m)

    waiting, late = [], []
    for group in groups:
        blocks = [m + odd for m in group for odd in (1, 0)]
        for m in blocks:
            arrive(m)
            lse[m] = jnp.zeros((rows, HD), jnp.float32)
        for i, m in enumerate(blocks):
            code = onehot_ref[xor(m)]
            for g in range(G):
                at = (i * G + g) * rows
                eg[at:at + rows] = code
        half = KV // 2
        compute(blocks, 0, half)
        settle([m for m in waiting if low_bit(m) <= 4])
        late += [m for m in waiting if low_bit(m) > 4]
        compute(blocks, half, KV)
        for m in blocks:
            if m % 2:
                send(m)
        waiting = group
    settle(sorted(late + waiting, key=low_bit))

    for bit in bits[:-1]:
        merge(0, bit)
    last = bits[-1]
    for copy in partner_copies(last):
        copy.wait_recv()
    w, level = blend(recv_l[last], lse[0])

    def finish(k, carry):
        base = pl.multiple_of(k * (G * HD), G * HD)
        for g in range(G):
            h = k * G + g
            at = pl.ds(base + g * HD, HD)
            a = recv_o[last, :, at].astype(jnp.float32)
            b = part[0, :, at].astype(jnp.float32)
            x = b + (a - b) * pick(w, h)
            mine = pl.ds(h, rows, stride=H)
            home = home_o[mine, :]
            w_home = 1.0 / (1.0 + jnp.exp2(pick(level, h) - home_l[mine, :]))
            out_ref[:, at] = (x + (home - x) * w_home).astype(jnp.bfloat16)
        return carry

    lax.fori_loop(0, KV, finish, 0, unroll=2)
    for m in range(1, n):
        gather_copy(m).wait_send()
        for copy in partner_copies(m):
            copy.wait_send()


def local(
    queries, new_keys, new_values, suffix_keys, suffix_values, suffix_lens,
    prefix_keys, prefix_values, page_table, prefix_id,
):
    n = lax.axis_size("seq")
    rows = queries.shape[0]
    slots = suffix_keys.shape[1]
    pages, page, width = prefix_keys.shape
    tokens = pages * page
    ids = lax.axis_index("seq") * pages + jnp.arange(pages, dtype=jnp.int32)
    hits = jnp.any(page_table[:, :, None] == ids[None, None, :], axis=1)
    prefixes = jnp.arange(NPREF, dtype=jnp.int32)
    label = jnp.sum(hits.astype(jnp.int32) * prefixes[:, None], axis=0)
    lanes = jnp.arange(HD, dtype=jnp.int32)
    barred = (lanes[None, :] < NPREF) & (lanes[None, :] != label[:, None])
    label_cols = jnp.where(barred, MASKED, 0.0).astype(jnp.bfloat16)
    label_cols = jnp.broadcast_to(label_cols[:, None, :], (pages, page, HD)).reshape(tokens, HD)
    onehot = (prefix_id.reshape(n, rows, 1) == lanes).astype(jnp.bfloat16)
    vmem = pl.BlockSpec(memory_space=pltpu.VMEM)
    hbm = pl.BlockSpec(memory_space=pl.ANY)
    smem = pl.BlockSpec(memory_space=pltpu.SMEM)
    bf16, f32 = jnp.bfloat16, jnp.float32
    dma = pltpu.SemaphoreType.DMA
    return pl.pallas_call(
        functools.partial(kernel, n),
        out_shape=jax.ShapeDtypeStruct((rows, H * HD), bf16),
        in_specs=[hbm, vmem, vmem, hbm, hbm, smem, hbm, hbm, vmem, vmem],
        out_specs=vmem,
        scratch_shapes=[
            pltpu.VMEM((n, rows, H * HD), bf16),
            pltpu.VMEM((rows, slots, width), bf16),
            pltpu.VMEM((rows, slots, width), bf16),
            pltpu.VMEM((tokens, width), bf16),
            pltpu.VMEM((tokens, width), bf16),
            pltpu.VMEM((n, rows, H * HD), bf16),
            pltpu.VMEM((n, rows, HD), f32),
            pltpu.VMEM((n, rows, H * HD), bf16),
            pltpu.VMEM((n, rows, HD), f32),
            pltpu.VMEM((4 * G * rows, HD), bf16),
            pltpu.VMEM((rows * H, HD), f32),
            pltpu.VMEM((rows * H, HD), f32),
            pltpu.VMEM((rows * H, HD), f32),
            dma((3,)),
            dma((2, rows)),
            dma((n,)), dma((n,)), dma((n,)), dma((n,)), dma((n,)), dma((n,)),
        ],
        compiler_params=pltpu.CompilerParams(
            collective_id=0, has_side_effects=True, vmem_limit_bytes=64 * 1024 * 1024 - 65536,
        ),
        name="step",
    )(
        queries, new_keys, new_values, suffix_keys, suffix_values, suffix_lens,
        prefix_keys.reshape(tokens, width), prefix_values.reshape(tokens, width),
        label_cols, onehot,
    )


def solution(mesh):
    return jax.shard_map(
        local,
        mesh=mesh,
        in_specs=(
            P(("grp", "seq"), None),
            P(("grp", "seq"), None),
            P(("grp", "seq"), None),
            P(("grp", "seq"), None, None),
            P(("grp", "seq"), None, None),
            P(("grp", "seq")),
            P(("grp", "seq"), None, None),
            P(("grp", "seq"), None, None),
            P("grp", None),
            P("grp"),
        ),
        out_specs=P(("grp", "seq"), None),
        check_vma=False,
    )
```
